32 devices in a mesh: dp: 16 (over z, x, core), tensor: 2 (over y).
Axes of the slice: x: 2, y: 2, z: 4, core: 2. Of those that a mesh axis runs over, the one named last changes fastest.
Arguments:
- block_input: bfloat16 [32, 577, 1024], P('dp'), may hold values from -6 to 6
- first_scale: float32 [1024], replicated, may hold values from 0.5 to 1.5
- first_shift: float32 [1024], replicated, may hold values from -3 to 3
- heads_weight: bfloat16 [1024, 3, 1024], P(None, None, 'tensor'), may hold values from -0.1875 to 0.1875
- heads_bias: float32 [2, 1024], P(None, 'tensor'), may hold values from -3 to 3
- mixing_weight: bfloat16 [1024, 1024], P('tensor'), may hold values from -0.75 to 0.75
- mixing_bias: float32 [1024], replicated, may hold values from -3 to 3
- second_scale: float32 [1024], replicated, may hold values from 0.5 to 1.5
- second_shift: float32 [1024], replicated, may hold values from -3 to 3
- expand_weight: bfloat16 [1024, 4096], P(None, 'tensor'), may hold values from -0.1875 to 0.1875
- expand_bias: float32 [4096], P('tensor'), may hold values from -3 to 3
- shrink_weight: bfloat16 [4096, 1024], P('tensor'), may hold values from -0.09375 to 0.09375
- shrink_bias: float32 [1024], replicated, may hold values from -3 to 3
- output_grad: bfloat16 [32, 577, 1024], P('dp'), may hold values from -6 to 6
Outputs:
- block_output: bfloat16 [32, 577, 1024], P('dp')
- input_grad: bfloat16 [32, 577, 1024], P('dp')
- heads_weight_grad: float32 [1024, 3, 1024], P(None, None, 'tensor')
- heads_bias_grad: float32 [2, 1024], P(None, 'tensor')
- mixing_weight_grad: float32 [1024, 1024], P('tensor')
- mixing_bias_grad: float32 [1024], replicated
- second_scale_grad: float32 [1024], replicated
- second_shift_grad: float32 [1024], replicated
- expand_weight_grad: float32 [1024, 4096], P(None, 'tensor')
- expand_bias_grad: float32 [4096], P('tensor')
- shrink_weight_grad: float32 [4096, 1024], P('tensor')
- shrink_bias_grad: float32 [1024], replicated
- first_scale_grad: float32 [1024], replicated
- first_shift_grad: float32 [1024], replicated
The draws below stay inside these ranges and needn't reach their ends.
All inputs are finite; a program needn't handle non-finite values.
Results may differ from the reference program's by a relative error of at most 0.012.
Values sent between devices are 32-bit elements; how exact they have to be, the bound alone decides.
A program may use at most 256 MiB of HBM per device.

```python
import math
import jax
import jax.numpy as jnp
from jax import lax

D = 1024
HEADS = 16
HEAD_DIM = 64
FF = 4096
SEQ = 577
IMAGES = 32


def block_scale(own_key, extent, shards, smallest, largest):
    loudness, own = 1.0, jax.random.fold_in(own_key, 6)
    for position, shards_of in shards:
        steps = jnp.exp(jax.random.uniform(jax.random.fold_in(own, position), (shards_of,), jnp.float32, smallest / len(shards), largest / len(shards)))
        loudness = loudness * jnp.repeat(steps, extent[position] // shards_of).reshape([-1 if axis == position else 1 for axis in range(len(extent))])
    return loudness


def gaussian(own_key, extent, scale, bound, cuts=(), dtype=jnp.bfloat16):
    drawn = jax.random.normal(own_key, extent, jnp.float32) * scale
    if len(cuts) > 0:
        drawn = block_scale(own_key, extent, cuts, -0.22, 0.18) * drawn
    return jnp.clip(drawn, min=-bound, max=bound).astype(dtype)


def setup_inputs(seed: int = 0) -> dict:
    key_list = jax.random.split(jax.random.key(seed), 15)
    return {
        "block_input": gaussian(key_list[0], (IMAGES, SEQ, D), 1.0, 6.0, ((0, 16),)),
        "first_scale": jnp.clip(1.0 + 0.1 * jax.random.normal(key_list[1], (D,), jnp.float32), 0.5, 1.5),
        "first_shift": gaussian(key_list[2], (D,), 0.5, 3.0, (), jnp.float32),
        "heads_weight": gaussian(key_list[3], (D, 3, D), D ** -0.5, 0.1875, ((2, 2),)),
        "heads_bias": gaussian(key_list[4], (2, D), 0.5, 3.0, ((1, 2),), jnp.float32),
        "mixing_weight": gaussian(key_list[5], (D, D), (D // 16) ** -0.5, 0.75, ((0, 2),)),
        "mixing_bias": gaussian(key_list[6], (D,), 0.5, 3.0, (), jnp.float32),
        "second_scale": jnp.clip(1.0 + 0.1 * jax.random.normal(key_list[7], (D,), jnp.float32), 0.5, 1.5),
        "second_shift": gaussian(key_list[8], (D,), 0.5, 3.0, (), jnp.float32),
        "expand_weight": gaussian(key_list[9], (D, FF), D ** -0.5, 0.1875, ((1, 2),)),
        "expand_bias": gaussian(key_list[10], (FF,), 0.5, 3.0, ((0, 2),), jnp.float32),
        "shrink_weight": gaussian(key_list[11], (FF, D), FF ** -0.5, 0.09375, ((0, 2),)),
        "shrink_bias": gaussian(key_list[12], (D,), 0.5, 3.0, (), jnp.float32),
        "output_grad": gaussian(key_list[13], (IMAGES, SEQ, D), 1.0, 6.0, ((0, 16),)),
    }


EPSILON = 1e-06

def normalize(values):
    center = values - lax.optimization_barrier(jnp.mean(values, axis=-1, keepdims=True))
    inverse = lax.rsqrt(lax.optimization_barrier(jnp.mean(center * center, axis=-1, keepdims=True)) + EPSILON)
    return (center * inverse, inverse)

def norm_back(grad_out, scale, normed, inverse):
    scaled = grad_out * scale
    return inverse * (scaled - lax.optimization_barrier(jnp.mean(scaled, axis=-1, keepdims=True)) - normed * lax.optimization_barrier(jnp.mean(scaled * normed, axis=-1, keepdims=True)))

def gelu_slope(pre_act):
    cumul = 0.5 * (1.0 + lax.erf(pre_act * 0.7071067811865476))
    return cumul + pre_act * jnp.exp(-0.5 * pre_act * pre_act) * 0.3989422804014327

def cross_dot(left_side, right_side):
    return lax.dot_general(left_side, right_side, (((0,), (0,)), ((), ())), preferred_element_type=jnp.float32)

def back_dot(left_side, right_side):
    return lax.dot_general(left_side, right_side, (((1,), (1,)), ((), ())), preferred_element_type=jnp.float32)

def one_image(params, image_in, image_grad):
    first_scale, first_shift, heads_weight, heads_bias, mixing_weight, mixing_bias, second_scale, second_shift, expand_weight, expand_bias, shrink_weight, shrink_bias = params
    factor = 1.0 / math.sqrt(HEAD_DIM)
    head_shape = (SEQ, HEADS, HEAD_DIM)
    flat_in = image_in.astype(jnp.float32)
    normed_one, inverse_one = normalize(flat_in)
    layer_one = (normed_one * first_scale + first_shift).astype(jnp.bfloat16)
    joined_weight = heads_weight.reshape(D, 3 * D)
    projected = jnp.dot(layer_one, joined_weight, preferred_element_type=jnp.float32).reshape(SEQ, 3, D)
    queries = (projected[:, 0] + heads_bias[0]).astype(jnp.bfloat16).reshape(head_shape)
    keys_all = projected[:, 1].astype(jnp.bfloat16).reshape(head_shape)
    values_all = (projected[:, 2] + heads_bias[1]).astype(jnp.bfloat16).reshape(head_shape)
    scores = jnp.einsum('qhd,khd->hqk', queries.astype(jnp.float32), keys_all.astype(jnp.float32)) * factor
    logsum = jax.nn.logsumexp(scores, axis=-1, keepdims=True)
    probs_low = jnp.exp(scores - logsum).astype(jnp.bfloat16)
    attended = jnp.einsum('hqk,khd->qhd', probs_low.astype(jnp.float32), values_all.astype(jnp.float32))
    attended = attended.astype(jnp.bfloat16).reshape(SEQ, D)
    hidden_one = flat_in + jnp.dot(attended, mixing_weight, preferred_element_type=jnp.float32) + mixing_bias
    normed_two, inverse_two = normalize(hidden_one)
    layer_two = (normed_two * second_scale + second_shift).astype(jnp.bfloat16)
    pre_act = jnp.dot(layer_two, expand_weight, preferred_element_type=jnp.float32) + expand_bias
    activated = jax.nn.gelu(pre_act, approximate=False).astype(jnp.bfloat16)
    block_output = (hidden_one + jnp.dot(activated, shrink_weight, preferred_element_type=jnp.float32) + shrink_bias).astype(jnp.bfloat16)
    upstream_wide = image_grad.astype(jnp.float32)
    shrink_grad = cross_dot(activated, image_grad)
    shrink_bias_grad = lax.optimization_barrier(jnp.sum(upstream_wide, axis=0))
    pre_grad = back_dot(image_grad, shrink_weight) * gelu_slope(pre_act)
    pre_low = pre_grad.astype(jnp.bfloat16)
    expand_bias_grad = lax.optimization_barrier(jnp.sum(pre_grad, axis=0))
    expand_grad = cross_dot(layer_two, pre_low)
    layer_two_grad = back_dot(pre_low, expand_weight)
    second_scale_grad = lax.optimization_barrier(jnp.sum(layer_two_grad * normed_two, axis=0))
    second_shift_grad = lax.optimization_barrier(jnp.sum(layer_two_grad, axis=0))
    hidden_grad = upstream_wide + norm_back(layer_two_grad, second_scale, normed_two, inverse_two)
    mixing_bias_grad = lax.optimization_barrier(jnp.sum(hidden_grad, axis=0))
    hidden_low = hidden_grad.astype(jnp.bfloat16)
    mixing_grad = cross_dot(attended, hidden_low)
    attended_grad = back_dot(hidden_low, mixing_weight).astype(jnp.bfloat16).reshape(head_shape)
    probs = jnp.exp(scores - logsum)
    values_grad = jnp.einsum('hqk,qhd->khd', probs.astype(jnp.bfloat16).astype(jnp.float32), attended_grad.astype(jnp.float32))
    probs_grad = jnp.einsum('qhd,khd->hqk', attended_grad.astype(jnp.float32), values_all.astype(jnp.float32))
    row_dot = lax.optimization_barrier(jnp.sum(probs * probs_grad, axis=-1, keepdims=True))
    score_low = (probs * (probs_grad - row_dot) * factor).astype(jnp.bfloat16).astype(jnp.float32)
    queries_grad = jnp.einsum('hqk,khd->qhd', score_low, keys_all.astype(jnp.float32))
    keys_grad = jnp.einsum('hqk,qhd->khd', score_low, queries.astype(jnp.float32))
    stacked = jnp.stack([queries_grad.reshape(SEQ, D), keys_grad.reshape(SEQ, D), values_grad.reshape(SEQ, D)], axis=1)
    heads_bias_grad = jnp.stack([lax.optimization_barrier(jnp.sum(stacked[:, 0], axis=0)), lax.optimization_barrier(jnp.sum(stacked[:, 2], axis=0))])
    stacked_low = stacked.astype(jnp.bfloat16).reshape(SEQ, 3 * D)
    heads_grad = cross_dot(layer_one, stacked_low).reshape(D, 3, D)
    layer_one_grad = back_dot(stacked_low, joined_weight)
    first_scale_grad = lax.optimization_barrier(jnp.sum(layer_one_grad * normed_one, axis=0))
    first_shift_grad = lax.optimization_barrier(jnp.sum(layer_one_grad, axis=0))
    input_grad = (hidden_grad + norm_back(layer_one_grad, first_scale, normed_one, inverse_one)).astype(jnp.bfloat16)
    grads = (heads_grad, heads_bias_grad, mixing_grad, mixing_bias_grad, second_scale_grad, second_shift_grad, expand_grad, expand_bias_grad, shrink_grad, shrink_bias_grad, first_scale_grad, first_shift_grad)
    return (block_output, input_grad, grads)

def reference(block_input, first_scale, first_shift, heads_weight, heads_bias, mixing_weight, mixing_bias, second_scale, second_shift, expand_weight, expand_bias, shrink_weight, shrink_bias, output_grad):
    params = (first_scale, first_shift, heads_weight, heads_bias, mixing_weight, mixing_bias, second_scale, second_shift, expand_weight, expand_bias, shrink_weight, shrink_bias)
    start = (jnp.zeros((D, 3, D), jnp.float32), jnp.zeros((2, D), jnp.float32), jnp.zeros((D, D), jnp.float32), jnp.zeros((D,), jnp.float32), jnp.zeros((D,), jnp.float32), jnp.zeros((D,), jnp.float32), jnp.zeros((D, FF), jnp.float32), jnp.zeros((FF,), jnp.float32), jnp.zeros((FF, D), jnp.float32), jnp.zeros((D,), jnp.float32), jnp.zeros((D,), jnp.float32), jnp.zeros((D,), jnp.float32))

    def step_image(carry, pair):
        image_out, image_back, grads = one_image(params, pair[0], pair[1])
        carry = jax.tree.map(lambda total, term: total + term, carry, grads)
        return (carry, (image_out, image_back))
    totals, (block_output, input_grad) = lax.scan(step_image, start, (block_input, output_grad))
    heads_grad, heads_bias_grad, mixing_grad, mixing_bias_grad, second_scale_grad, second_shift_grad, expand_grad, expand_bias_grad, shrink_grad, shrink_bias_grad, first_scale_grad, first_shift_grad = totals
    return (block_output, input_grad, heads_grad, heads_bias_grad, mixing_grad, mixing_bias_grad, second_scale_grad, second_shift_grad, expand_grad, expand_bias_grad, shrink_grad, shrink_bias_grad, first_scale_grad, first_shift_grad)
```

```python
import functools
import math

import jax
import jax.numpy as jnp
from jax import lax
from jax.experimental import pallas as pl
from jax.experimental.pallas import tpu as pltpu
from jax.sharding import PartitionSpec as P

HEAD_DIM = 64
PAIR = 2 * HEAD_DIM
EPSILON = 1e-06
QUERIES = 128
LANES = 128
f32 = jnp.float32
bf16 = jnp.bfloat16


def dot(left, right):
    return jnp.dot(left, right, preferred_element_type=f32)


def nt_dot(left, right):
    return lax.dot_general(left, right, (((1,), (1,)), ((), ())), preferred_element_type=f32)


def tn_dot(left, right):
    return lax.dot_general(left, right, (((0,), (0,)), ((), ())), preferred_element_type=f32)


def cost(flops, nbytes, trans=0):
    return pl.CostEstimate(flops=flops, bytes_accessed=nbytes, transcendentals=trans)


def normalize(values):
    center = values - jnp.mean(values, axis=-1, keepdims=True)
    inverse = lax.rsqrt(jnp.mean(center * center, axis=-1, keepdims=True) + EPSILON)
    return center * inverse, inverse


def norm_back(grad_out, scale, normed, inverse):
    scaled = grad_out * scale
    return inverse * (
        scaled
        - jnp.mean(scaled, axis=-1, keepdims=True)
        - normed * jnp.mean(scaled * normed, axis=-1, keepdims=True)
    )


def pad_rows(target, source):
    rows, length = target.shape[0], source.shape[0]
    edge = length // 8 * 8
    if edge < rows:
        target[pl.ds(edge, rows - edge), :] = jnp.zeros((rows - edge, target.shape[1]), f32)
    target[pl.ds(0, length), :] = source.astype(f32)


def stack_heads(block, scale):
    lane = lax.broadcasted_iota(jnp.int32, block.shape, 1)
    block = block * jnp.asarray(scale, block.dtype)
    zero = jnp.zeros_like(block)
    return jnp.concatenate(
        [jnp.where(lane < HEAD_DIM, block, zero), jnp.where(lane < HEAD_DIM, zero, block)], axis=0
    )


def unstack_heads(stacked):
    return jnp.concatenate([stacked[:HEAD_DIM, :QUERIES], stacked[HEAD_DIM:, QUERIES:]], axis=0)


def fill_rows(target, source):
    rows = source.shape[0]
    target[pl.ds(0, rows), :] = source
    rest = target.shape[0] - rows
    if rest > 0:
        target[pl.ds(rows, rest), :] = jnp.zeros((rest, target.shape[1]), target.dtype)


def attend_kernel(
    length, chunks, input_ref, weight_ref, bias_ref, scale_ref, shift_ref,
    layer_ref, qkv_ref, out_ref, wide_ref, logsum_ref, block, queries, result,
):
    rows = layer_ref.shape[0]

    @pl.when(pl.program_id(0) == 0)
    def _():
        pad_rows(block, input_ref[...])
        normed, _ = normalize(block[...])
        layer_ref[...] = (normed * scale_ref[...] + shift_ref[...]).astype(bf16)

    qkv_ref[...] = (dot(layer_ref[...], weight_ref[...]) + bias_ref[...]).astype(bf16)
    fill_rows(queries, qkv_ref[:, 0:PAIR])
    keys = qkv_ref[:, PAIR : 2 * PAIR]
    values = qkv_ref[:, 2 * PAIR : 3 * PAIR]

    def body(step, carry):
        at = pl.ds(pl.multiple_of(step * QUERIES, QUERIES), QUERIES)
        stacked = stack_heads(queries[at, :], 1.0 / math.sqrt(HEAD_DIM))
        scores = nt_dot(keys, stacked)
        row = lax.broadcasted_iota(jnp.int32, scores.shape, 0)
        scores = jnp.where(row < length, scores, -1e30)
        top = jnp.max(scores, axis=0, keepdims=True)
        powers = jnp.exp(scores - top)
        total = jnp.sum(powers, axis=0, keepdims=True)
        probs = (powers * (1.0 / total)).astype(bf16)
        logsum_ref[step] = top + jnp.log(total)
        mixed = unstack_heads(tn_dot(values, probs))
        result[at, :] = mixed.T.astype(bf16)
        return carry

    lax.fori_loop(0, chunks, body, 0, unroll=True)
    low = result[pl.ds(0, rows), :]
    out_ref[...] = low
    wide_ref[...] = low.astype(f32)


def attend(image, rows, block_input, joined, joined_bias, scale, shift):
    _, length, width = block_input.shape
    pairs = joined.shape[1] // (3 * PAIR)
    chunks = -(-rows // QUERIES)
    pair_block = pl.BlockSpec((rows, PAIR), lambda j: (0, j))
    vector = pl.BlockSpec((1, width), lambda j: (0, 0))
    return pl.pallas_call(
        functools.partial(attend_kernel, length, chunks),
        grid=(pairs,),
        in_specs=[
            pl.BlockSpec((None, length, width), lambda j: (image, 0, 0)),
            pl.BlockSpec((width, 3 * PAIR), lambda j: (0, j)),
            pl.BlockSpec((1, 3 * PAIR), lambda j: (0, j)),
            vector,
            vector,
        ],
        out_specs=[
            pl.BlockSpec((rows, width), lambda j: (0, 0)),
            pl.BlockSpec((rows, 3 * PAIR), lambda j: (0, j)),
            pair_block,
            pair_block,
            pl.BlockSpec((None, chunks, 1, 2 * QUERIES), lambda j: (j, 0, 0, 0)),
        ],
        out_shape=[
            jax.ShapeDtypeStruct((rows, width), bf16),
            jax.ShapeDtypeStruct((rows, pairs * 3 * PAIR), bf16),
            jax.ShapeDtypeStruct((rows, pairs * PAIR), bf16),
            jax.ShapeDtypeStruct((rows, pairs * PAIR), f32),
            jax.ShapeDtypeStruct((pairs, chunks, 1, 2 * QUERIES), f32),
        ],
        scratch_shapes=[
            pltpu.VMEM((rows, width), f32),
            pltpu.VMEM((chunks * QUERIES, PAIR), bf16),
            pltpu.VMEM((chunks * QUERIES, PAIR), bf16),
        ],
        cost_estimate=cost(10_000_000_000, 10_000_000),
        name="attend",
    )(block_input, joined, joined_bias, scale, shift)


def attend_back_kernel(
    length, chunks, pairs, own_ref, other_ref, hidden_ref, upstream_ref, mixing_ref, qkv_ref,
    logsum_ref, joined_ref, input_ref, scale_ref,
    grad_ref, low_ref, out_ref, qbias_ref, vbias_ref, partial_ref, sums_ref, first_ref,
    block, queries, grads, query_out, key_sum, value_sum, stacked_all,
):
    pair = pl.program_id(0)
    rows = qkv_ref.shape[0]
    factor = 1.0 / math.sqrt(HEAD_DIM)

    @pl.when(pair == 0)
    def _():
        normed, inverse = normalize(hidden_ref[...])
        layer_grad = own_ref[...] + other_ref[...]
        upstream = upstream_ref[...].astype(f32)
        grad = upstream + norm_back(layer_grad, scale_ref[...], normed, inverse)
        grad_ref[...] = grad
        low_ref[...] = grad.astype(bf16)
        sums_ref[0:1, :] = jnp.sum(layer_grad * normed, axis=0, keepdims=True)
        sums_ref[1:2, :] = jnp.sum(layer_grad, axis=0, keepdims=True)
        sums_ref[2:3, :] = jnp.sum(grad, axis=0, keepdims=True)
        sums_ref[3:4, :] = jnp.sum(upstream, axis=0, keepdims=True)

    fill_rows(queries, qkv_ref[:, 0:PAIR])
    fill_rows(grads, nt_dot(low_ref[...], mixing_ref[...]).astype(bf16))
    keep = lax.broadcasted_iota(jnp.int32, (rows, PAIR), 0) < length
    empty = jnp.zeros((rows, PAIR), bf16)
    keys = jnp.where(keep, qkv_ref[:, PAIR : 2 * PAIR], empty)
    values = jnp.where(keep, qkv_ref[:, 2 * PAIR : 3 * PAIR], empty)
    key_sum[...] = jnp.zeros_like(key_sum)
    value_sum[...] = jnp.zeros_like(value_sum)

    def body(step, bias):
        at = pl.ds(pl.multiple_of(step * QUERIES, QUERIES), QUERIES)
        stacked = stack_heads(queries[at, :], factor)
        upstream = stack_heads(grads[at, :], 1.0)
        probs = jnp.exp(nt_dot(keys, stacked) - logsum_ref[step])
        probs_grad = nt_dot(values, upstream)
        value_sum[...] += dot(probs.astype(bf16), upstream)
        product = probs * probs_grad
        row_dot = jnp.sum(product, axis=0, keepdims=True)
        score = (product - probs * row_dot).astype(bf16)
        key_sum[...] += dot(score, stacked)
        query_grad = unstack_heads(tn_dot(keys, score)).T * factor
        query_out[at, :] = query_grad.astype(bf16)
        return bias + jnp.sum(query_grad, axis=0, keepdims=True)

    qbias_ref[...] = lax.fori_loop(0, chunks, body, jnp.zeros((1, PAIR), f32), unroll=True)
    wide = jnp.zeros((rows, PAIR), f32)
    value_grad = jnp.where(keep, value_sum[...], wide)
    vbias_ref[...] = jnp.sum(value_grad, axis=0, keepdims=True)
    out_ref[:, 0:PAIR] = query_out[pl.ds(0, rows), :]
    out_ref[:, PAIR : 2 * PAIR] = jnp.where(keep, key_sum[...], wide).astype(bf16)
    out_ref[:, 2 * PAIR : 3 * PAIR] = value_grad.astype(bf16)
    stacked_all[:, pl.ds(pl.multiple_of(pair * 3 * PAIR, LANES), 3 * PAIR)] = out_ref[...]

    @pl.when(pair == pairs - 1)
    def _():
        partial = nt_dot(stacked_all[...], joined_ref[...])
        partial_ref[...] = partial
        pad_rows(block, input_ref[...])
        normed, _ = normalize(block[...])
        first_ref[0:1, :] = jnp.sum(partial * normed, axis=0, keepdims=True)
        first_ref[1:2, :] = jnp.sum(partial, axis=0, keepdims=True)


def attend_back(image, own, other, hidden, upstream, mixing, qkv, logsum, joined, block_input, scale):
    rows, width = own.shape
    length = block_input.shape[1]
    pairs = joined.shape[1] // (3 * PAIR)
    chunks = -(-rows // QUERIES)
    full = pl.BlockSpec((rows, width), lambda j: (0, 0))
    stack = pl.BlockSpec((rows, 3 * PAIR), lambda j: (0, j))
    bias = pl.BlockSpec((1, PAIR), lambda j: (0, j))
    return pl.pallas_call(
        functools.partial(attend_back_kernel, length, chunks, pairs),
        grid=(pairs,),
        in_specs=[
            full,
            full,
            full,
            full,
            pl.BlockSpec((PAIR, width), lambda j: (j, 0)),
            stack,
            pl.BlockSpec((None, chunks, 1, 2 * QUERIES), lambda j: (j, 0, 0, 0)),
            pl.BlockSpec(joined.shape, lambda j: (0, 0)),
            pl.BlockSpec((None, length, width), lambda j: (image, 0, 0)),
            pl.BlockSpec((1, width), lambda j: (0, 0)),
        ],
        out_specs=[
            full,
            full,
            stack,
            bias,
            bias,
            full,
            pl.BlockSpec((4, width), lambda j: (0, 0)),
            pl.BlockSpec((2, width), lambda j: (0, 0)),
        ],
        out_shape=[
            jax.ShapeDtypeStruct((rows, width), f32),
            jax.ShapeDtypeStruct((rows, width), bf16),
            jax.ShapeDtypeStruct((rows, pairs * 3 * PAIR), bf16),
            jax.ShapeDtypeStruct((1, pairs * PAIR), f32),
            jax.ShapeDtypeStruct((1, pairs * PAIR), f32),
            jax.ShapeDtypeStruct((rows, width), f32),
            jax.ShapeDtypeStruct((4, width), f32),
            jax.ShapeDtypeStruct((2, width), f32),
        ],
        scratch_shapes=[pltpu.VMEM((rows, width), f32)]
        + [pltpu.VMEM((chunks * QUERIES, PAIR), bf16)] * 3
        + [pltpu.VMEM((rows, PAIR), f32)] * 2
        + [pltpu.VMEM((rows, pairs * 3 * PAIR), bf16)],
        cost_estimate=cost(12_000_000_000, 20_000_000),
        name="attend_back",
    )(own, other, hidden, upstream, mixing, qkv, logsum, joined, block_input, scale)


def gather_kernel(place_ref, own_ref, near_ref, far_ref, out_ref):
    half = near_ref.shape[0]
    own = place_ref[0] * 2 * half
    other = (1 - place_ref[0]) * 2 * half
    out_ref[pl.ds(pl.multiple_of(own, LANES), 2 * half), :] = own_ref[...]
    near = other + place_ref[1] * half
    far = other + (1 - place_ref[1]) * half
    out_ref[pl.ds(pl.multiple_of(near, LANES), half), :] = near_ref[...].astype(bf16)
    out_ref[pl.ds(pl.multiple_of(far, LANES), half), :] = far_ref[...].astype(bf16)


def gather_weight(place, own, near, far):
    whole = pl.BlockSpec(memory_space=pltpu.VMEM)
    return pl.pallas_call(
        gather_kernel,
        in_specs=[pl.BlockSpec(memory_space=pltpu.SMEM), whole, whole, whole],
        out_specs=whole,
        out_shape=jax.ShapeDtypeStruct((2 * own.shape[0], own.shape[1]), bf16),
        cost_estimate=cost(1_000_000, 6_000_000),
        name="gather_weight",
    )(place, own, near, far)


def feed_kernel(
    place_ref, input_ref, own_ref, other_ref, mixing_ref, mixing_bias_ref, scale_ref, shift_ref,
    upstream_ref, expand_ref, bias_ref, shrink_ref,
    hidden_ref, layer_ref, grad_ref, act_ref, low_ref, sum_ref, shrunk_ref, partial_ref,
    both, block,
):
    tile = pl.program_id(0)
    rows = layer_ref.shape[0]

    @pl.when(tile == 0)
    def _():
        width = own_ref.shape[1]
        own = place_ref[0] * width
        other = (1 - place_ref[0]) * width
        both[:, pl.ds(pl.multiple_of(own, LANES), width)] = own_ref[...]
        both[:, pl.ds(pl.multiple_of(other, LANES), width)] = other_ref[...].astype(bf16)
        pad_rows(block, input_ref[...])
        mixed = block[...] + dot(both[...], mixing_ref[...]) + mixing_bias_ref[...]
        hidden_ref[...] = mixed
        normed, _ = normalize(mixed)
        layer_ref[...] = (normed * scale_ref[...] + shift_ref[...]).astype(bf16)
        pad_rows(block, upstream_ref[...])
        grad_ref[...] = block[...].astype(bf16)

    cut = (rows // 32) * 16
    expand, shrink, bias = expand_ref[...], shrink_ref[...], bias_ref[...]
    total = jnp.zeros(bias.shape, f32)
    for low, high in ((0, cut), (cut, rows)):
        part = pl.ds(low, high - low)
        pre_act = dot(layer_ref[part, :], expand) + bias
        back = nt_dot(grad_ref[part, :], shrink)
        cumul = 0.5 * (1.0 + lax.erf(pre_act * 0.7071067811865476))
        slope = cumul + pre_act * jnp.exp(-0.5 * pre_act * pre_act) * 0.3989422804014327
        act = (pre_act * cumul).astype(bf16)
        act_ref[part, :] = act
        pre_grad = back * slope
        total = total + jnp.sum(pre_grad, axis=0, keepdims=True)
        pre_low = pre_grad.astype(bf16)
        low_ref[part, :] = pre_low
        shrunk = dot(act, shrink)
        partial = nt_dot(pre_low, expand)

        @pl.when(tile == 0)
        def _():
            shrunk_ref[part, :] = shrunk
            partial_ref[part, :] = partial

        @pl.when(tile > 0)
        def _():
            shrunk_ref[part, :] += shrunk
            partial_ref[part, :] += partial

    sum_ref[...] = total


def feed(
    image, place, block_input, own, other, mixing, mixing_bias, scale, shift, upstream,
    expand, bias, shrink,
):
    rows = own.shape[0]
    _, length, width = block_input.shape
    hidden = expand.shape[1]
    tile = math.gcd(hidden, 1024)
    full = pl.BlockSpec((rows, width), lambda j: (0, 0))
    half = pl.BlockSpec((rows, own.shape[1]), lambda j: (0, 0))
    vector = pl.BlockSpec((1, width), lambda j: (0, 0))
    picture = pl.BlockSpec((None, length, width), lambda j: (image, 0, 0))
    block = pl.BlockSpec((rows, tile), lambda j: (0, j))
    row = pl.BlockSpec((1, tile), lambda j: (0, j))
    return pl.pallas_call(
        feed_kernel,
        grid=(hidden // tile,),
        in_specs=[
            pl.BlockSpec(memory_space=pltpu.SMEM),
            picture,
            half,
            half,
            pl.BlockSpec(mixing.shape, lambda j: (0, 0)),
            vector,
            vector,
            vector,
            picture,
            pl.BlockSpec((width, tile), lambda j: (0, j)),
            row,
            pl.BlockSpec((tile, width), lambda j: (j, 0)),
        ],
        out_specs=[full, full, full, block, block, row, full, full],
        out_shape=[
            jax.ShapeDtypeStruct((rows, width), f32),
            jax.ShapeDtypeStruct((rows, width), bf16),
            jax.ShapeDtypeStruct((rows, width), bf16),
            jax.ShapeDtypeStruct((rows, hidden), bf16),
            jax.ShapeDtypeStruct((rows, hidden), bf16),
            jax.ShapeDtypeStruct((1, hidden), f32),
            jax.ShapeDtypeStruct((rows, width), f32),
            jax.ShapeDtypeStruct((rows, width), f32),
        ],
        scratch_shapes=[pltpu.VMEM((rows, width), bf16), pltpu.VMEM((rows, width), f32)],
        cost_estimate=cost(11_000_000_000, 25_000_000),
        name="feed",
    )(place, block_input, own, other, mixing, mixing_bias, scale, shift, upstream, expand, bias, shrink)


def weight_kernel(images, per, core_ref, *refs):
    lefts, rights = refs[:images], refs[images : 2 * images]
    keep_ref, send_ref, work = refs[2 * images :]
    total = tn_dot(lefts[0][...], rights[0][...])
    for left, right in zip(lefts[1:], rights[1:]):
        total = total + tn_dot(left[...], right[...])
    work[...] = total
    core = core_ref[0]
    share = keep_ref.shape[1]
    for chip in range(per):
        keep_ref[chip] = work[pl.ds(pl.multiple_of((2 * chip + core) * share, 8), share), :]
        send_ref[chip] = work[pl.ds(pl.multiple_of((2 * chip + 1 - core) * share, 8), share), :]


def weight_grad(lefts, rights, core, chips):
    rows, height = lefts[0].shape
    width = rights[0].shape[1]
    share = height // (2 * chips)
    block = max(LANES, 2 * share)
    per = block // (2 * share)
    images = len(lefts)
    tiles = jax.ShapeDtypeStruct((chips, share, width), f32)
    tile_spec = pl.BlockSpec((per, share, width), lambda i, c: (i, 0, 0))
    return pl.pallas_call(
        functools.partial(weight_kernel, images, per),
        grid_spec=pltpu.PrefetchScalarGridSpec(
            num_scalar_prefetch=1,
            grid=(height // block,),
            in_specs=[pl.BlockSpec((rows, block), lambda i, c: (0, i))] * images
            + [pl.BlockSpec((rows, width), lambda i, c: (0, 0))] * images,
            out_specs=[tile_spec, tile_spec],
            scratch_shapes=[pltpu.VMEM((block, width), f32)],
        ),
        out_shape=[tiles, tiles],
        cost_estimate=cost(2 * images * rows * height * width * 3 // 2, 4 * height * width),
        name="weight_grad",
    )(core, *lefts, *rights)


def chip_of(place, chips):
    place = (place + 4 * chips) % chips
    upper = place // (chips // 2)
    return (1 - upper) * 2 * place + upper * (2 * (chips - 1 - place) + 1)

def ring_kernel(chips, count, cuts, *refs):
    keep, sent, out = refs[:count], refs[count:2*count], refs[2*count:3*count]
    other, slot = refs[3*count:4*count], refs[4*count:5*count]
    swap_send, swap_recv, ring_send, ring_recv, pass_send, pass_recv, give_send, give_recv, store = refs[5*count:]
    me = lax.axis_index("dp")
    core, chip = me % 2, me // 2
    column = chip % 2
    place = (1 - column) * (chip // 2) + column * (chips - 1 - chip // 2)
    turn = 1 - 2 * core
    ahead = 2 * chip_of(place + turn, chips) + core
    behind = 2 * chip_of(place - turn, chips) + core
    across = 2 * chip + 1 - core
    barrier = pltpu.get_barrier_semaphore()
    for device in (ahead, behind, across):
        pl.semaphore_signal(barrier, inc=1, device_id={"dp": device}, device_id_type=pl.DeviceIdType.MESH)
    pl.semaphore_wait(barrier, 3)
    def remote(src, dst, send, recv, device):
        return pltpu.make_async_remote_copy(src_ref=src, dst_ref=dst, send_sem=send, recv_sem=recv,
            device_id={"dp": device}, device_id_type=pl.DeviceIdType.MESH)
    def swap_copy(w, s):
        tile = chip_of(place + turn * (s + 1), chips)
        return remote(sent[w].at[tile], other[w].at[tile], swap_send.at[w, s], swap_recv.at[w, s], across)
    def swap_wait(w, s):
        tile = chip_of(place - turn * (s + 1), chips)
        remote(sent[w].at[tile], other[w].at[tile], swap_send.at[w, s], swap_recv.at[w, s], across).wait_recv()
    pieces = [(w, c) for c in range(max(cuts)) for w in range(count) if c < cuts[w]]
    def part(w, c):
        n = slot[w].shape[1] // cuts[w]
        return pl.ds(c * n, n)
    def ring_copy(w, c, s):
        return remote(slot[w].at[s, part(w, c)], slot[w].at[s + 1, part(w, c)],
                      ring_send.at[w, c, s], ring_recv.at[w, c, s], ahead)
    def out_at(w, c, s):
        return out[w].at[chip_of(place - turn * s, chips), core, part(w, c)]
    def start_swap(s, carry):
        for w in range(count):
            swap_copy(w, s).start()
        return carry
    lax.fori_loop(0, chips, start_swap, 0)
    for w in range(count):
        swap_wait(w, 0)
    tile0 = chip_of(place - turn, chips)
    for w, c in pieces:
        slot[w][0, part(w, c)] = keep[w][tile0, part(w, c)] + other[w][tile0, part(w, c)]
        ring_copy(w, c, 0).start()
    def reduce_step(s, carry):
        tile = chip_of(place - turn * (s + 1), chips)
        for w in range(count):
            swap_wait(w, s)
        for w, c in pieces:
            ring_copy(w, c, s - 1).wait_recv()
            slot[w][s, part(w, c)] = slot[w][s, part(w, c)] + (keep[w][tile, part(w, c)] + other[w][tile, part(w, c)])
            @pl.when(s < chips - 1)
            def _():
                ring_copy(w, c, s).start()
            @pl.when(s == chips - 1)
            def _():
                own = slot[w].at[chips - 1, part(w, c)]
                remote(own, out_at(w, c, 0), pass_send.at[w, c, 0], pass_recv.at[w, c, 0], ahead).start()
                remote(own, out_at(w, c, 0), give_send.at[w, c, 0], give_recv.at[w, c, 0], across).start()
                pltpu.make_async_copy(own, out_at(w, c, 0), store.at[w, c]).start()
        return carry
    lax.fori_loop(1, chips, reduce_step, 0)
    def pass_copy(w, c, s):
        return remote(out_at(w, c, s), out_at(w, c, s), pass_send.at[w, c, s], pass_recv.at[w, c, s], ahead)
    def give_copy(w, c, s):
        return remote(out_at(w, c, s), out_at(w, c, s), give_send.at[w, c, s], give_recv.at[w, c, s], across)
    def gather_step(s, carry):
        for w, c in pieces:
            at = out_at(w, c, s)
            remote(at, at, pass_send.at[w, c, s - 1], pass_recv.at[w, c, s - 1], ahead).wait_recv()
            @pl.when(s < chips - 1)
            def _():
                pass_copy(w, c, s).start()
            give_copy(w, c, s).start()
        return carry
    lax.fori_loop(1, chips, gather_step, 0)
    def drain(s, carry):
        for w in range(count):
            swap_copy(w, s).wait_send()
        for w, c in pieces:
            @pl.when(s < chips - 1)
            def _():
                ring_copy(w, c, s).wait_send()
                pass_copy(w, c, s).wait_send()
            give_copy(w, c, s).wait_send()
            theirs = out[w].at[chip_of(place + turn * s, chips), 1 - core, part(w, c)]
            remote(theirs, theirs, give_send.at[w, c, s], give_recv.at[w, c, s], across).wait_recv()
        return carry
    lax.fori_loop(0, chips, drain, 0)
    for w, c in pieces:
        pltpu.make_async_copy(slot[w].at[chips - 1, part(w, c)], out_at(w, c, 0), store.at[w, c]).wait()

def ring_sum(tiles, collective_id, cut=4):
    count = len(tiles)
    chips = tiles[0][0].shape[0]
    cuts = []
    for keep, _ in tiles:
        share = keep.shape[1]
        cuts.append(max(c for c in range(1, cut + 1) if share % (8 * c) == 0))
    hbm = pl.BlockSpec(memory_space=pl.ANY); vmem = pl.BlockSpec(memory_space=pltpu.VMEM)
    dma = lambda *s: pltpu.SemaphoreType.DMA(s)
    most = max(cuts)
    outs = pl.pallas_call(
        functools.partial(ring_kernel, chips, count, tuple(cuts)),
        in_specs=[vmem] * count + [hbm] * count,
        out_specs=[hbm] * count,
        out_shape=[jax.ShapeDtypeStruct((chips, 2) + k.shape[1:], f32) for k, _ in tiles],
        scratch_shapes=[pltpu.VMEM(k.shape, f32) for k, _ in tiles] * 2
        + [dma(count, chips)] * 2 + [dma(count, most, chips)] * 6 + [dma(count, most)],
        compiler_params=pltpu.CompilerParams(collective_id=collective_id, has_side_effects=True),
        name="ring_sum",
    )(*[k for k, _ in tiles], *[s for _, s in tiles])
    return [o.reshape(-1, o.shape[-1]) for o in outs]


def output_kernel(hidden_ref, own_ref, other_ref, bias_ref, *out):
    length = out[-1].shape[0]
    part = pl.ds(0, length)
    out[-1][...] = (
        hidden_ref[part, :] + (own_ref[part, :] + other_ref[part, :]) + bias_ref[...]
    ).astype(bf16)


def input_kernel(grad_ref, own_ref, other_ref, input_ref, scale_ref, *out):
    length = out[-1].shape[0]
    part = pl.ds(0, length)
    normed, inverse = normalize(input_ref[...].astype(f32))
    layer_grad = own_ref[part, :] + other_ref[part, :]
    out[-1][...] = (
        grad_ref[part, :] + norm_back(layer_grad, scale_ref[...], normed, inverse)
    ).astype(bf16)


def finish(kernel, name, image, shape, operands, before):
    images, length, width = shape
    picture = pl.BlockSpec((None, length, width), lambda j: (image, 0, 0))

    def spec(array):
        return picture if array.ndim == 3 else pl.BlockSpec(array.shape, lambda j: (0, 0))

    extra = [] if before is None else [before]
    return pl.pallas_call(
        kernel,
        grid=(1,),
        in_specs=[spec(a) for a in operands] + [pl.BlockSpec(memory_space=pl.ANY)] * len(extra),
        out_specs=picture,
        out_shape=jax.ShapeDtypeStruct(shape, bf16),
        input_output_aliases={len(operands): 0} if extra else {},
        cost_estimate=cost(10_000_000, 10_000_000),
        name=name,
    )(*operands, *extra)


def swap(array):
    return lax.ppermute(array, "tensor", [(0, 1), (1, 0)])


def on_device(
    block_input,
    first_scale,
    first_shift,
    heads_weight,
    heads_bias,
    mixing_weight,
    mixing_bias,
    second_scale,
    second_shift,
    expand_weight,
    expand_bias,
    shrink_weight,
    shrink_bias,
    output_grad,
):
    images, length, width = block_input.shape
    local = heads_weight.shape[2]
    pairs = local // PAIR
    hidden = expand_weight.shape[1]
    rows = -(-length // 16) * 16
    size = lax.axis_size("dp")
    chips = size // 2
    owner = lax.axis_index("tensor")
    core = lax.axis_index("dp") % 2
    cores = [(i, i ^ 1) for i in range(size)]
    place = jnp.stack([owner, core]).astype(jnp.int32)
    which = core.astype(jnp.int32).reshape(1)
    first_scale, first_shift, mixing_bias, second_scale, second_shift, shrink_bias = (
        v.reshape(1, width)
        for v in (first_scale, first_shift, mixing_bias, second_scale, second_shift, shrink_bias)
    )

    half = mixing_weight.shape[0] // 2
    piece = swap(lax.dynamic_slice_in_dim(mixing_weight, core * half, half, 0).astype(f32))
    piece_two = lax.ppermute(piece, "dp", cores)
    full_mixing = gather_weight(place, mixing_weight, piece, piece_two)

    joined = (
        heads_weight.reshape(width, 3, pairs, PAIR).transpose(0, 2, 1, 3).reshape(width, 3 * local)
    )
    zero_bias = jnp.zeros((pairs, PAIR), f32)
    joined_bias = jnp.stack(
        [heads_bias[0].reshape(pairs, PAIR), zero_bias, heads_bias[1].reshape(pairs, PAIR)], axis=1
    ).reshape(1, 3 * local)

    each_image = range(images)
    layer_one, qkv, attended, wide, logsum = zip(
        *[
            attend(i, rows, block_input, joined, joined_bias, first_scale, first_shift)
            for i in each_image
        ]
    )
    hidden_one, layer_two, upstream, activated, pre_low, expand_sums, shrunk, partial_two = zip(
        *[
            feed(
                i, place, block_input, attended[i], swap(wide[i]), full_mixing, mixing_bias,
                second_scale, second_shift, output_grad, expand_weight,
                expand_bias.reshape(1, hidden), shrink_weight,
            )
            for i in each_image
        ]
    )
    shrink_tiles = weight_grad(activated, upstream, which, chips)
    expand_tiles = weight_grad(layer_two, pre_low, which, chips)
    (shrink_full,) = ring_sum([shrink_tiles], 1)

    (
        hidden_grad, hidden_low, stacked, query_bias, value_bias, partial_one, sums_two, sums_one,
    ) = zip(
        *[
            attend_back(
                i, partial_two[i], swap(partial_two[i]), hidden_one[i], upstream[i], mixing_weight,
                qkv[i], logsum[i], joined, block_input, second_scale,
            )
            for i in each_image
        ]
    )
    heads_tiles = weight_grad(layer_one, stacked, which, chips)
    mixing_tiles = weight_grad(attended, hidden_low, which, chips)
    small = jnp.concatenate(
        [
            sum(query_bias).reshape(-1),
            sum(value_bias).reshape(-1),
            sum(expand_sums).reshape(-1),
            sum(sums_two).reshape(-1),
            sum(sums_one).reshape(-1),
        ]
    )
    each = -(-small.shape[0] // size)
    chunk = -(-each // (8 * LANES)) * 8 * LANES
    small_tiles = jnp.pad(small, (0, each * size - small.shape[0])).reshape(size, each)
    small_tiles = jnp.pad(small_tiles, ((0, 0), (0, chunk - each))).reshape(
        chips, 2, chunk // LANES, LANES
    )
    small_pair = (
        lax.dynamic_index_in_dim(small_tiles, core, 1, keepdims=False),
        lax.dynamic_index_in_dim(small_tiles, 1 - core, 1, keepdims=False),
    )
    heads_full, expand_full, mixing_full, small_full = ring_sum(
        [heads_tiles, expand_tiles, mixing_tiles, small_pair], 2
    )
    heads_full = (
        heads_full.reshape(width, pairs, 3, PAIR).transpose(0, 2, 1, 3).reshape(width, 3, local)
    )
    small = small_full.reshape(size, chunk)[:, :each].reshape(-1)

    block_output = input_grad = None
    for i in each_image:
        block_output = finish(
            output_kernel, "output", i, block_input.shape,
            [hidden_one[i], shrunk[i], swap(shrunk[i]), shrink_bias], block_output,
        )
    for i in each_image:
        input_grad = finish(
            input_kernel, "input", i, block_input.shape,
            [hidden_grad[i], partial_one[i], swap(partial_one[i]), block_input, first_scale],
            input_grad,
        )

    parts, at = [], 0
    for count in (2 * local, hidden) + 6 * (width,):
        parts.append(small[at : at + count])
        at += count
    first = jnp.stack(parts[6:8])
    first = first + swap(first)
    return (
        block_output,
        input_grad,
        heads_full,
        parts[0].reshape(2, local),
        mixing_full,
        parts[4],
        parts[2],
        parts[3],
        expand_full,
        parts[1],
        shrink_full,
        parts[5],
        first[0],
        first[1],
    )


def solution(mesh):
    placed = (
        P("dp", None, None),
        P(),
        P(),
        P(None, None, "tensor"),
        P(None, "tensor"),
        P("tensor", None),
        P(),
        P(),
        P(),
        P(None, "tensor"),
        P("tensor"),
        P("tensor", None),
        P(),
        P("dp", None, None),
    )
    return jax.shard_map(
        on_device,
        mesh=mesh,
        in_specs=placed,
        out_specs=(
            P("dp", None, None),
            P("dp", None, None),
            P(None, None, "tensor"),
            P(None, "tensor"),
            P("tensor", None),
            P(),
            P(),
            P(),
            P(None, "tensor"),
            P("tensor"),
            P("tensor", None),
            P(),
            P(),
            P(),
        ),
        check_vma=False,
    )
```

```python
import functools
import math

import jax
import jax.numpy as jnp
from jax import lax
from jax.experimental import pallas as pl
from jax.experimental.pallas import tpu as pltpu
from jax.sharding import PartitionSpec as P


HEAD_DIM = 64
PAIR = 2 * HEAD_DIM
EPSILON = 1e-06
QUERIES = 128
LANES = 128
f32 = jnp.float32
bf16 = jnp.bfloat16


def dot(left, right):
    return jnp.dot(left, right, preferred_element_type=f32)


def nt_dot(left, right):
    return lax.dot_general(left, right, (((1,), (1,)), ((), ())), preferred_element_type=f32)


def tn_dot(left, right):
    return lax.dot_general(left, right, (((0,), (0,)), ((), ())), preferred_element_type=f32)


def cost(flops, nbytes, trans=0):
    return pl.CostEstimate(flops=flops, bytes_accessed=nbytes, transcendentals=trans)


def normalize(values):
    center = values - jnp.mean(values, axis=-1, keepdims=True)
    inverse = lax.rsqrt(jnp.mean(center * center, axis=-1, keepdims=True) + EPSILON)
    return center * inverse, inverse


def norm_back(grad_out, scale, normed, inverse):
    scaled = grad_out * scale
    return inverse * (
        scaled
        - jnp.mean(scaled, axis=-1, keepdims=True)
        - normed * jnp.mean(scaled * normed, axis=-1, keepdims=True)
    )


def pad_rows(target, source):
    rows, length = target.shape[0], source.shape[0]
    edge = length // 8 * 8
    if edge < rows:
        target[pl.ds(edge, rows - edge), :] = jnp.zeros((rows - edge, target.shape[1]), f32)
    target[pl.ds(0, length), :] = source.astype(f32)


def stack_heads(block, scale):
    lane = lax.broadcasted_iota(jnp.int32, block.shape, 1)
    block = block * jnp.asarray(scale, block.dtype)
    zero = jnp.zeros_like(block)
    return jnp.concatenate(
        [jnp.where(lane < HEAD_DIM, block, zero), jnp.where(lane < HEAD_DIM, zero, block)], axis=0
    )


def unstack_heads(stacked):
    return jnp.concatenate([stacked[:HEAD_DIM, :QUERIES], stacked[HEAD_DIM:, QUERIES:]], axis=0)


def fill_rows(target, source):
    rows = source.shape[0]
    target[pl.ds(0, rows), :] = source
    rest = target.shape[0] - rows
    if rest > 0:
        target[pl.ds(rows, rest), :] = jnp.zeros((rest, target.shape[1]), target.dtype)


def attend_kernel(
    length, chunks, input_ref, weight_ref, bias_ref, scale_ref, shift_ref,
    layer_ref, qkv_ref, out_ref, wide_ref, logsum_ref, block, queries, result,
):
    rows = layer_ref.shape[0]

    @pl.when(pl.program_id(0) == 0)
    def _():
        pad_rows(block, input_ref[...])
        normed, _ = normalize(block[...])
        layer_ref[...] = (normed * scale_ref[...] + shift_ref[...]).astype(bf16)

    qkv_ref[...] = (dot(layer_ref[...], weight_ref[...]) + bias_ref[...]).astype(bf16)
    fill_rows(queries, qkv_ref[:, 0:PAIR])
    keys = qkv_ref[:, PAIR : 2 * PAIR]
    values = qkv_ref[:, 2 * PAIR : 3 * PAIR]

    def body(step, carry):
        at = pl.ds(pl.multiple_of(step * QUERIES, QUERIES), QUERIES)
        stacked = stack_heads(queries[at, :], 1.0 / math.sqrt(HEAD_DIM))
        scores = nt_dot(keys, stacked)
        row = lax.broadcasted_iota(jnp.int32, scores.shape, 0)
        scores = jnp.where(row < length, scores, -1e30)
        top = jnp.max(scores, axis=0, keepdims=True)
        powers = jnp.exp(scores - top)
        total = jnp.sum(powers, axis=0, keepdims=True)
        probs = (powers * (1.0 / total)).astype(bf16)
        logsum_ref[step] = top + jnp.log(total)
        mixed = unstack_heads(tn_dot(values, probs))
        result[at, :] = mixed.T.astype(bf16)
        return carry

    lax.fori_loop(0, chunks, body, 0, unroll=True)
    low = result[pl.ds(0, rows), :]
    out_ref[...] = low
    wide_ref[...] = low.astype(f32)


def attend(image, rows, block_input, joined, joined_bias, scale, shift):
    _, length, width = block_input.shape
    pairs = joined.shape[1] // (3 * PAIR)
    chunks = -(-rows // QUERIES)
    pair_block = pl.BlockSpec((rows, PAIR), lambda j: (0, j))
    vector = pl.BlockSpec((1, width), lambda j: (0, 0))
    return pl.pallas_call(
        functools.partial(attend_kernel, length, chunks),
        grid=(pairs,),
        in_specs=[
            pl.BlockSpec((None, length, width), lambda j: (image, 0, 0)),
            pl.BlockSpec((width, 3 * PAIR), lambda j: (0, j)),
            pl.BlockSpec((1, 3 * PAIR), lambda j: (0, j)),
            vector,
            vector,
        ],
        out_specs=[
            pl.BlockSpec((rows, width), lambda j: (0, 0)),
            pl.BlockSpec((rows, 3 * PAIR), lambda j: (0, j)),
            pair_block,
            pair_block,
            pl.BlockSpec((None, chunks, 1, 2 * QUERIES), lambda j: (j, 0, 0, 0)),
        ],
        out_shape=[
            jax.ShapeDtypeStruct((rows, width), bf16),
            jax.ShapeDtypeStruct((rows, pairs * 3 * PAIR), bf16),
            jax.ShapeDtypeStruct((rows, pairs * PAIR), bf16),
            jax.ShapeDtypeStruct((rows, pairs * PAIR), f32),
            jax.ShapeDtypeStruct((pairs, chunks, 1, 2 * QUERIES), f32),
        ],
        scratch_shapes=[
            pltpu.VMEM((rows, width), f32),
            pltpu.VMEM((chunks * QUERIES, PAIR), bf16),
            pltpu.VMEM((chunks * QUERIES, PAIR), bf16),
        ],
        cost_estimate=cost(10_000_000_000, 10_000_000),
        name="attend",
    )(block_input, joined, joined_bias, scale, shift)


def attend_back_kernel(
    length, chunks, pairs, own_ref, other_ref, hidden_ref, upstream_ref, mixing_ref, qkv_ref,
    logsum_ref, joined_ref, input_ref, scale_ref,
    grad_ref, low_ref, out_ref, qbias_ref, vbias_ref, partial_ref, sums_ref, first_ref,
    block, queries, grads, query_out, key_sum, value_sum, stacked_all, mark=None,
):
    pair = pl.program_id(0)
    rows = qkv_ref.shape[0]
    factor = 1.0 / math.sqrt(HEAD_DIM)

    @pl.when(pair == 0)
    def _():
        normed, inverse = normalize(hidden_ref[...])
        layer_grad = own_ref[...] + other_ref[...]
        upstream = upstream_ref[...].astype(f32)
        grad = upstream + norm_back(layer_grad, scale_ref[...], normed, inverse)
        grad_ref[...] = grad
        low_ref[...] = grad.astype(bf16)
        sums_ref[0:1, :] = jnp.sum(layer_grad * normed, axis=0, keepdims=True)
        sums_ref[1:2, :] = jnp.sum(layer_grad, axis=0, keepdims=True)
        sums_ref[2:3, :] = jnp.sum(grad, axis=0, keepdims=True)
        sums_ref[3:4, :] = jnp.sum(upstream, axis=0, keepdims=True)

    fill_rows(queries, qkv_ref[:, 0:PAIR])
    fill_rows(grads, nt_dot(low_ref[...], mixing_ref[...]).astype(bf16))
    keep = lax.broadcasted_iota(jnp.int32, (rows, PAIR), 0) < length
    empty = jnp.zeros((rows, PAIR), bf16)
    keys = jnp.where(keep, qkv_ref[:, PAIR : 2 * PAIR], empty)
    values = jnp.where(keep, qkv_ref[:, 2 * PAIR : 3 * PAIR], empty)
    key_sum[...] = jnp.zeros_like(key_sum)
    value_sum[...] = jnp.zeros_like(value_sum)

    def body(step, bias):
        if mark is not None:
            mark(step)
        at = pl.ds(step * QUERIES, QUERIES)
        stacked = stack_heads(queries[at, :], factor)
        upstream = stack_heads(grads[at, :], 1.0)
        probs = jnp.exp(nt_dot(keys, stacked) - logsum_ref[step])
        probs_grad = nt_dot(values, upstream)
        value_sum[...] += dot(probs.astype(bf16), upstream)
        product = probs * probs_grad
        row_dot = jnp.sum(product, axis=0, keepdims=True)
        score = (product - probs * row_dot).astype(bf16)
        key_sum[...] += dot(score, stacked)
        query_grad = unstack_heads(tn_dot(keys, score)).T * factor
        query_out[at, :] = query_grad.astype(bf16)
        return bias + jnp.sum(query_grad, axis=0, keepdims=True)

    bias = jnp.zeros((1, PAIR), f32)
    for step in range(chunks):
        bias = body(step, bias)
    qbias_ref[...] = bias
    wide = jnp.zeros((rows, PAIR), f32)
    value_grad = jnp.where(keep, value_sum[...], wide)
    vbias_ref[...] = jnp.sum(value_grad, axis=0, keepdims=True)
    out_ref[:, 0:PAIR] = query_out[pl.ds(0, rows), :]
    out_ref[:, PAIR : 2 * PAIR] = jnp.where(keep, key_sum[...], wide).astype(bf16)
    out_ref[:, 2 * PAIR : 3 * PAIR] = value_grad.astype(bf16)
    stacked_all[:, pl.ds(pl.multiple_of(pair * 3 * PAIR, LANES), 3 * PAIR)] = out_ref[...]

    @pl.when(pair == pairs - 1)
    def _():
        partial = nt_dot(stacked_all[...], joined_ref[...])
        partial_ref[...] = partial
        pad_rows(block, input_ref[...])
        normed, _ = normalize(block[...])
        first_ref[0:1, :] = jnp.sum(partial * normed, axis=0, keepdims=True)
        first_ref[1:2, :] = jnp.sum(partial, axis=0, keepdims=True)


def attend_back(
    image, own, other, hidden, upstream, mixing, qkv, logsum, joined, block_input, scale,
    own_tile, chips, collective_id,
):
    rows, width = own.shape
    length = block_input.shape[1]
    pairs = joined.shape[1] // (3 * PAIR)
    chunks = -(-rows // QUERIES)
    once = dict(pipeline_mode=pl.Buffered(1))
    full = pl.BlockSpec((rows, width), lambda j: (0, 0), **once)
    out = pl.BlockSpec((rows, width), lambda j: (0, 0))
    stack = pl.BlockSpec((rows, 3 * PAIR), lambda j: (0, j))
    bias = pl.BlockSpec((1, PAIR), lambda j: (0, j))
    in_specs = [
        full,
        full,
        full,
        full,
        pl.BlockSpec((PAIR, width), lambda j: (j, 0)),
        stack,
        pl.BlockSpec((None, chunks, 1, 2 * QUERIES), lambda j: (j, 0, 0, 0)),
        pl.BlockSpec(joined.shape, lambda j: (0, 0), **once),
        pl.BlockSpec((None, length, width), lambda j: (image, 0, 0), **once),
        pl.BlockSpec((1, width), lambda j: (0, 0)),
    ]
    out_specs = [
        out,
        out,
        stack,
        bias,
        bias,
        out,
        pl.BlockSpec((4, width), lambda j: (0, 0)),
        pl.BlockSpec((2, width), lambda j: (0, 0)),
    ]
    out_shape = [
        jax.ShapeDtypeStruct((rows, width), f32),
        jax.ShapeDtypeStruct((rows, width), bf16),
        jax.ShapeDtypeStruct((rows, pairs * 3 * PAIR), bf16),
        jax.ShapeDtypeStruct((1, pairs * PAIR), f32),
        jax.ShapeDtypeStruct((1, pairs * PAIR), f32),
        jax.ShapeDtypeStruct((rows, width), f32),
        jax.ShapeDtypeStruct((4, width), f32),
        jax.ShapeDtypeStruct((2, width), f32),
    ]
    scratch = (
        [pltpu.VMEM((rows, width), f32)]
        + [pltpu.VMEM((chunks * QUERIES, PAIR), bf16)] * 3
        + [pltpu.VMEM((rows, PAIR), f32)] * 2
        + [pltpu.VMEM((rows, pairs * 3 * PAIR), bf16)]
    )
    operands = [own, other, hidden, upstream, mixing, qkv, logsum, joined, block_input, scale]
    ins, outs, shapes, extra = Gather.specs(own_tile, chips)
    kernel = functools.partial(attend_back_kernel, length, chunks, pairs)
    return pl.pallas_call(
        riding(kernel, len(in_specs), len(out_specs), len(scratch), pairs, chunks),
        grid=(pairs,),
        in_specs=in_specs + ins,
        out_specs=out_specs + outs,
        out_shape=out_shape + shapes,
        scratch_shapes=scratch + extra,
        compiler_params=pltpu.CompilerParams(collective_id=collective_id, has_side_effects=True),
        cost_estimate=cost(40_000_000_000, 20_000_000),
        name="attend_back",
    )(*operands, own_tile)


def gather_kernel(place_ref, own_ref, near_ref, far_ref, out_ref):
    half = near_ref.shape[0]
    own = place_ref[0] * 2 * half
    other = (1 - place_ref[0]) * 2 * half
    out_ref[pl.ds(pl.multiple_of(own, LANES), 2 * half), :] = own_ref[...]
    near = other + place_ref[1] * half
    far = other + (1 - place_ref[1]) * half
    out_ref[pl.ds(pl.multiple_of(near, LANES), half), :] = near_ref[...].astype(bf16)
    out_ref[pl.ds(pl.multiple_of(far, LANES), half), :] = far_ref[...].astype(bf16)


def gather_weight(place, own, near, far):
    whole = pl.BlockSpec(memory_space=pltpu.VMEM)
    return pl.pallas_call(
        gather_kernel,
        in_specs=[pl.BlockSpec(memory_space=pltpu.SMEM), whole, whole, whole],
        out_specs=whole,
        out_shape=jax.ShapeDtypeStruct((2 * own.shape[0], own.shape[1]), bf16),
        cost_estimate=cost(1_000_000, 6_000_000),
        name="gather_weight",
    )(place, own, near, far)


def feed_kernel(
    place_ref, input_ref, own_ref, other_ref, mixing_ref, mixing_bias_ref, scale_ref, shift_ref,
    upstream_ref, expand_ref, bias_ref, shrink_ref,
    hidden_ref, layer_ref, grad_ref, act_ref, low_ref, sum_ref, shrunk_ref, partial_ref,
    both, block,
):
    tile = pl.program_id(0)
    rows = layer_ref.shape[0]

    @pl.when(tile == 0)
    def _():
        width = own_ref.shape[1]
        own = place_ref[0] * width
        other = (1 - place_ref[0]) * width
        both[:, pl.ds(pl.multiple_of(own, LANES), width)] = own_ref[...]
        both[:, pl.ds(pl.multiple_of(other, LANES), width)] = other_ref[...].astype(bf16)
        pad_rows(block, input_ref[...])
        mixed = block[...] + dot(both[...], mixing_ref[...]) + mixing_bias_ref[...]
        hidden_ref[...] = mixed
        normed, _ = normalize(mixed)
        layer_ref[...] = (normed * scale_ref[...] + shift_ref[...]).astype(bf16)
        pad_rows(block, upstream_ref[...])
        grad_ref[...] = block[...].astype(bf16)

    cut = (rows // 32) * 16
    expand, shrink, bias = expand_ref[...], shrink_ref[...], bias_ref[...]
    total = jnp.zeros(bias.shape, f32)
    for low, high in ((0, cut), (cut, rows)):
        part = pl.ds(low, high - low)
        pre_act = dot(layer_ref[part, :], expand) + bias
        back = nt_dot(grad_ref[part, :], shrink)
        cumul = 0.5 * (1.0 + lax.erf(pre_act * 0.7071067811865476))
        slope = cumul + pre_act * jnp.exp(-0.5 * pre_act * pre_act) * 0.3989422804014327
        act = (pre_act * cumul).astype(bf16)
        act_ref[part, :] = act
        pre_grad = back * slope
        total = total + jnp.sum(pre_grad, axis=0, keepdims=True)
        pre_low = pre_grad.astype(bf16)
        low_ref[part, :] = pre_low
        shrunk = dot(act, shrink)
        partial = nt_dot(pre_low, expand)

        @pl.when(tile == 0)
        def _():
            shrunk_ref[part, :] = shrunk
            partial_ref[part, :] = partial

        @pl.when(tile > 0)
        def _():
            shrunk_ref[part, :] += shrunk
            partial_ref[part, :] += partial

    sum_ref[...] = total


def feed(
    image, place, block_input, own, other, mixing, mixing_bias, scale, shift, upstream,
    expand, bias, shrink,
):
    rows = own.shape[0]
    _, length, width = block_input.shape
    hidden = expand.shape[1]
    tile = math.gcd(hidden, 1024)
    full = pl.BlockSpec((rows, width), lambda j: (0, 0))
    half = pl.BlockSpec((rows, own.shape[1]), lambda j: (0, 0))
    vector = pl.BlockSpec((1, width), lambda j: (0, 0))
    picture = pl.BlockSpec((None, length, width), lambda j: (image, 0, 0))
    block = pl.BlockSpec((rows, tile), lambda j: (0, j))
    row = pl.BlockSpec((1, tile), lambda j: (0, j))
    return pl.pallas_call(
        feed_kernel,
        grid=(hidden // tile,),
        in_specs=[
            pl.BlockSpec(memory_space=pltpu.SMEM),
            picture,
            half,
            half,
            pl.BlockSpec(mixing.shape, lambda j: (0, 0)),
            vector,
            vector,
            vector,
            picture,
            pl.BlockSpec((width, tile), lambda j: (0, j)),
            row,
            pl.BlockSpec((tile, width), lambda j: (j, 0)),
        ],
        out_specs=[full, full, full, block, block, row, full, full],
        out_shape=[
            jax.ShapeDtypeStruct((rows, width), f32),
            jax.ShapeDtypeStruct((rows, width), bf16),
            jax.ShapeDtypeStruct((rows, width), bf16),
            jax.ShapeDtypeStruct((rows, hidden), bf16),
            jax.ShapeDtypeStruct((rows, hidden), bf16),
            jax.ShapeDtypeStruct((1, hidden), f32),
            jax.ShapeDtypeStruct((rows, width), f32),
            jax.ShapeDtypeStruct((rows, width), f32),
        ],
        scratch_shapes=[pltpu.VMEM((rows, width), bf16), pltpu.VMEM((rows, width), f32)],
        cost_estimate=cost(11_000_000_000, 25_000_000),
        name="feed",
    )(place, block_input, own, other, mixing, mixing_bias, scale, shift, upstream, expand, bias, shrink)


def chip_of(place, chips):
    place = (place + 4 * chips) % chips
    upper = place // (chips // 2)
    return (1 - upper) * 2 * place + upper * (2 * (chips - 1 - place) + 1)


def remote(source, target, send, receive, device):
    return pltpu.make_async_remote_copy(
        src_ref=source,
        dst_ref=target,
        send_sem=send,
        recv_sem=receive,
        device_id={"dp": device},
        device_id_type=pl.DeviceIdType.MESH,
    )


class Place:
    def __init__(self, chips):
        me = lax.axis_index("dp")
        self.chips = chips
        self.core = me % 2
        chip = me // 2
        column = chip % 2
        self.place = (1 - column) * (chip // 2) + column * (chips - 1 - chip // 2)
        self.turn = 1 - 2 * self.core
        self.ahead = 2 * chip_of(self.place + self.turn, chips) + self.core
        self.behind = 2 * chip_of(self.place - self.turn, chips) + self.core
        self.across = 2 * chip + 1 - self.core

    def barrier(self):
        semaphore = pltpu.get_barrier_semaphore()
        for device in (self.ahead, self.behind, self.across):
            pl.semaphore_signal(
                semaphore, inc=1, device_id={"dp": device}, device_id_type=pl.DeviceIdType.MESH
            )
        pl.semaphore_wait(semaphore, 3)

    def chip_at(self, steps):
        return chip_of(self.place + self.turn * steps, self.chips)


def cuts_of(share):
    return max(c for c in range(1, 5) if share % (8 * c) == 0)


class Reduce:
    def __init__(self, make, own, keep, sent, other, slot, swap_send, swap_recv, ring_send, ring_recv):
        self.make = make
        self.keep, self.sent, self.own, self.other, self.slot = keep, sent, own, other, slot
        self.swap_sems, self.ring_sems = (swap_send, swap_recv), (ring_send, ring_recv)
        self.chips, share = slot.shape[0], slot.shape[1]
        self.cuts = ring_send.shape[0]
        self.piece = share // self.cuts
        self.at = Place(self.chips)

    @staticmethod
    def scratch(chips, share, width):
        dma = pltpu.SemaphoreType.DMA
        cuts = cuts_of(share)
        return [pltpu.VMEM((chips, share, width), f32)] * 4 + (
            [dma((chips,))] * 2 + [dma((cuts, chips - 1))] * 2
        )

    def part(self, cut):
        return pl.ds(pl.multiple_of(cut * self.piece, 8), self.piece)

    def swap(self, step, sign):
        tile = self.at.chip_at(sign * (step + 1))
        send, receive = self.swap_sems
        return remote(
            self.sent.at[tile], self.other.at[tile], send.at[step], receive.at[step], self.at.across
        )

    def ring(self, cut, step):
        send, receive = self.ring_sems
        part = self.part(cut)
        return remote(
            self.slot.at[step, part],
            self.slot.at[step + 1, part],
            send.at[cut, step],
            receive.at[cut, step],
            self.at.ahead,
        )

    def prepare(self, step):
        @pl.when(2 * (step + 1) < self.chips)
        def _():
            self.make(self.at.chip_at(step + 1))
            self.swap(step, 1).start()
            self.make(self.at.chip_at(-(step + 1)))

        @pl.when(2 * (step + 1) == self.chips)
        def _():
            self.make(self.at.chip_at(step + 1))
            self.swap(step, 1).start()

        @pl.when((2 * (step + 1) > self.chips) & (step < self.chips - 1))
        def _():
            self.swap(step, 1).start()

        @pl.when(step == self.chips - 1)
        def _():
            self.make(self.at.chip_at(0))
            self.swap(step, 1).start()

    def unit(self, step, cut):
        part = self.part(cut)
        tile = self.at.chip_at(-(step + 1))

        @pl.when(step == 0)
        def _():
            self.slot[0, part] = self.keep[tile, part] + self.other[tile, part]

        @pl.when(step > 0)
        def _():
            self.ring(cut, step - 1).wait_recv()
            self.slot[step, part] += self.keep[tile, part] + self.other[tile, part]

        @pl.when(step < self.chips - 1)
        def _():
            self.ring(cut, step).start()

        @pl.when(step == self.chips - 1)
        def _():
            self.own[part] = self.slot[step, part]

    def run(self):
        self.at.barrier()
        self.prepare(0)

        def body(step, carry):
            @pl.when(step < self.chips - 1)
            def _():
                self.prepare(step + 1)

            self.swap(step, -1).wait_recv()
            for cut in range(self.cuts):
                self.unit(step, cut)
            return carry

        lax.fori_loop(0, self.chips, body, 0)

        def sent(step, carry):
            self.swap(step, 1).wait_send()

            @pl.when(step < self.chips - 1)
            def _():
                for cut in range(self.cuts):
                    self.ring(cut, step).wait_send()

            return carry

        lax.fori_loop(0, self.chips, sent, 0)


class Gather:
    def __init__(self, own, out, pass_send, pass_recv, give_send, give_recv, store):
        self.own, self.out, self.store = own, out, store
        self.pass_sems, self.give_sems = (pass_send, pass_recv), (give_send, give_recv)
        self.chips = out.shape[0]
        self.cuts = store.shape[0]
        self.piece = own.shape[0] // self.cuts
        self.units = (self.chips - 1) * self.cuts
        self.at = Place(self.chips)

    @staticmethod
    def specs(own, chips):
        share, width = own.shape
        cuts = cuts_of(share)
        dma = pltpu.SemaphoreType.DMA
        return (
            [pl.BlockSpec(memory_space=pltpu.VMEM)],
            [pl.BlockSpec(memory_space=pl.ANY)],
            [jax.ShapeDtypeStruct((chips, 2, share, width), f32)],
            [dma((cuts, chips - 1))] * 2 + [dma((cuts, chips))] * 2 + [dma((cuts,))],
        )

    def part(self, cut):
        return pl.ds(pl.multiple_of(cut * self.piece, 8), self.piece)

    def tile(self, cut, behind):
        return self.out.at[self.at.chip_at(-behind), self.at.core, self.part(cut)]

    def onward(self, source, cut, behind):
        send, receive = self.pass_sems
        return remote(
            source, self.tile(cut, behind), send.at[cut, behind], receive.at[cut, behind], self.at.ahead
        )

    def give(self, source, cut, behind):
        send, receive = self.give_sems
        return remote(
            source, self.tile(cut, behind), send.at[cut, behind], receive.at[cut, behind], self.at.across
        )

    def keep(self, cut):
        return pltpu.make_async_copy(
            self.own.at[self.part(cut)], self.tile(cut, 0), self.store.at[cut]
        )

    def start(self):
        self.at.barrier()

        def body(cut, carry):
            source = self.own.at[self.part(cut)]
            self.onward(source, cut, 0).start()
            self.give(source, cut, 0).start()
            self.keep(cut).start()
            return carry

        lax.fori_loop(0, self.cuts, body, 0)

    def unit(self, index):
        behind, cut = 1 + index // self.cuts, index % self.cuts
        here = self.tile(cut, behind)
        send, receive = self.pass_sems
        remote(
            here, here, send.at[cut, behind - 1], receive.at[cut, behind - 1], self.at.ahead
        ).wait_recv()

        @pl.when(behind < self.chips - 1)
        def _():
            self.onward(here, cut, behind).start()

        self.give(here, cut, behind).start()

    def run(self, first, last):
        def body(index, carry):
            self.unit(index)
            return carry

        lax.fori_loop(first, last, body, 0)

    def finish(self):
        send, receive = self.give_sems

        def body(index, carry):
            cut, behind = index // self.chips, index % self.chips
            here = self.tile(cut, behind)

            @pl.when(behind < self.chips - 1)
            def _():
                self.onward(here, cut, behind).wait_send()

            self.give(here, cut, behind).wait_send()
            theirs = self.out.at[self.at.chip_at(behind), 1 - self.at.core, self.part(cut)]
            remote(
                theirs, theirs, send.at[cut, behind], receive.at[cut, behind], self.at.across
            ).wait_recv()

            @pl.when(behind == 0)
            def _():
                self.keep(cut).wait()

            return carry

        lax.fori_loop(0, self.cuts * self.chips, body, 0)


def riding(kernel, inputs, outputs, scratch, steps, marks):
    def body(*refs):
        ins, own, rest = refs[:inputs], refs[inputs], refs[inputs + 1 :]
        outs, full, rest = rest[:outputs], rest[outputs], rest[outputs + 1 :]
        own_scratch, extra = rest[:scratch], rest[scratch:]
        rider = Gather(own, full, *extra)
        step = pl.program_id(0)
        total = steps * marks

        @pl.when(step == 0)
        def _():
            rider.start()

        def mark(number):
            at = step * marks + number
            rider.run(at * rider.units // total, (at + 1) * rider.units // total)

        kernel(*ins, *outs, *own_scratch, mark=mark)

        @pl.when(step == steps - 1)
        def _():
            rider.finish()

    return body


def gather_kernel_alone(own, out, *sems):
    rider = Gather(own, out, *sems)
    rider.start()
    rider.run(0, rider.units)
    rider.finish()


def gather_alone(own, chips, collective_id):
    ins, outs, shapes, scratch = Gather.specs(own, chips)
    return pl.pallas_call(
        gather_kernel_alone,
        in_specs=ins,
        out_specs=outs,
        out_shape=shapes,
        scratch_shapes=scratch,
        compiler_params=pltpu.CompilerParams(collective_id=collective_id, has_side_effects=True),
        cost_estimate=cost(40_000_000_000, 10_000_000),
        name="gather",
    )(own)[0]


def product(lefts, rights, block, chip, per):
    at = pl.ds(pl.multiple_of(chip // per * block, LANES), block)
    total = tn_dot(lefts[0][:, at], rights[0][...])
    for left, right in zip(lefts[1:], rights[1:]):
        total = total + tn_dot(left[:, at], right[...])
    return total


def block_of(height, chips):
    block = max(LANES, height // chips)
    return block, block * chips // height


def weight_kernel(images, *refs):
    lefts, rights = refs[:images], refs[images : 2 * images]
    own, keep, sent, other, slot, work, *sems = refs[2 * images :]
    chips, share = slot.shape[0], slot.shape[1]
    block, per = block_of(lefts[0].shape[1], chips)
    core = lax.axis_index("dp") % 2

    def make(chip):
        work[...] = product(lefts, rights, block, chip, per)
        first = chip % per * 2
        keep[chip] = work[pl.ds(pl.multiple_of((first + core) * share, 8), share), :]
        sent[chip] = work[pl.ds(pl.multiple_of((first + 1 - core) * share, 8), share), :]

    Reduce(make, own, keep, sent, other, slot, *sems).run()


def reducing(kernel, operands, chips, share, width, work, collective_id):
    arrays = Reduce.scratch(chips, share, width)
    whole = pl.BlockSpec(memory_space=pltpu.VMEM)
    return pl.pallas_call(
        kernel,
        in_specs=[whole] * len(operands),
        out_specs=whole,
        out_shape=jax.ShapeDtypeStruct((share, width), f32),
        scratch_shapes=arrays[:4] + work + arrays[4:],
        compiler_params=pltpu.CompilerParams(collective_id=collective_id, has_side_effects=True),
        cost_estimate=cost(40_000_000_000, 20_000_000),
    )(*operands)


def weight_grad(lefts, rights, chips, collective_id):
    height, width = lefts[0].shape[1], rights[0].shape[1]
    block, _ = block_of(height, chips)
    return reducing(
        functools.partial(weight_kernel, len(lefts)), [*lefts, *rights], chips,
        height // (2 * chips), width, [pltpu.VMEM((block, width), f32)], collective_id,
    )


def heads_kernel(images, *refs):
    layers, stacks, attended, lows = (refs[k * images : (k + 1) * images] for k in range(4))
    small, own, keep, sent, other, slot, work, work_two, *sems = refs[4 * images :]
    chips, part = slot.shape[0], slot.shape[2]
    core = lax.axis_index("dp") % 2
    block, per = block_of(layers[0].shape[1], chips)
    block_two, per_two = block_of(attended[0].shape[1], chips)
    share, mixing = block // (2 * per), block_two // (2 * per_two)

    def split(source, chip, per, share, columns, rows, lanes):
        first = chip % per * 2
        for target, which in ((keep, core), (sent, 1 - core)):
            target[chip, rows, lanes] = source[
                pl.ds(pl.multiple_of((first + which) * share, 8), share), columns
            ]

    def make(chip):
        work[...] = product(layers, stacks, block, chip, per)
        for which in range(3):
            for pair in range(part // PAIR):
                split(
                    work, chip, per, share, pl.ds((3 * pair + which) * PAIR, PAIR),
                    pl.ds(which * share, share), pl.ds(pair * PAIR, PAIR),
                )
        work_two[...] = product(attended, lows, block_two, chip, per_two)
        at = 3 * share
        for piece in range(work_two.shape[1] // part):
            split(
                work_two, chip, per_two, mixing, pl.ds(piece * part, part), pl.ds(at, mixing),
                pl.ds(0, part),
            )
            at += mixing
        rest = pl.ds(at, keep.shape[1] - at)
        keep[chip, rest, :] = small[chip, core]
        sent[chip, rest, :] = small[chip, 1 - core]

    Reduce(make, own, keep, sent, other, slot, *sems).run()


def heads_grad(layers, stacks, attended, lows, small, chips, collective_id):
    height, wide = layers[0].shape[1], stacks[0].shape[1]
    part = wide // 3
    mixing_height, mixing_width = attended[0].shape[1], lows[0].shape[1]
    share = (height * 3 + mixing_height * mixing_width // part) // (2 * chips) + small.shape[2]
    work = [
        pltpu.VMEM((block_of(height, chips)[0], wide), f32),
        pltpu.VMEM((block_of(mixing_height, chips)[0], mixing_width), f32),
    ]
    return reducing(
        functools.partial(heads_kernel, len(layers)),
        [*layers, *stacks, *attended, *lows, small], chips, share, part, work, collective_id,
    )


def output_kernel(hidden_ref, own_ref, other_ref, bias_ref, *out):
    length = out[-1].shape[0]
    part = pl.ds(0, length)
    out[-1][...] = (
        hidden_ref[part, :] + (own_ref[part, :] + other_ref[part, :]) + bias_ref[...]
    ).astype(bf16)


def input_kernel(grad_ref, own_ref, other_ref, input_ref, scale_ref, *out):
    length = out[-1].shape[0]
    part = pl.ds(0, length)
    normed, inverse = normalize(input_ref[...].astype(f32))
    layer_grad = own_ref[part, :] + other_ref[part, :]
    out[-1][...] = (
        grad_ref[part, :] + norm_back(layer_grad, scale_ref[...], normed, inverse)
    ).astype(bf16)


def finish(kernel, image, shape, operands, before):
    _, length, width = shape
    picture = pl.BlockSpec((None, length, width), lambda j: (image, 0, 0))

    def spec(array):
        return picture if array.ndim == 3 else pl.BlockSpec(array.shape, lambda j: (0, 0))

    extra = [] if before is None else [before]
    return pl.pallas_call(
        kernel,
        grid=(1,),
        in_specs=[spec(a) for a in operands] + [pl.BlockSpec(memory_space=pl.ANY)] * len(extra),
        out_specs=picture,
        out_shape=jax.ShapeDtypeStruct(shape, bf16),
        input_output_aliases={len(operands): 0} if extra else {},
        cost_estimate=cost(10_000_000, 10_000_000),
    )(*operands, *extra)


def swap(array):
    return lax.ppermute(array, "tensor", [(0, 1), (1, 0)])


def layer(
    block_input,
    first_scale,
    first_shift,
    heads_weight,
    heads_bias,
    mixing_weight,
    mixing_bias,
    second_scale,
    second_shift,
    expand_weight,
    expand_bias,
    shrink_weight,
    shrink_bias,
    output_grad,
):
    images, length, width = block_input.shape
    local = heads_weight.shape[2]
    pairs = local // PAIR
    hidden = expand_weight.shape[1]
    rows = -(-length // 16) * 16
    size = lax.axis_size("dp")
    chips = size // 2
    owner = lax.axis_index("tensor")
    core = lax.axis_index("dp") % 2
    cores = [(i, i ^ 1) for i in range(size)]
    place = jnp.stack([owner, core]).astype(jnp.int32)
    first_scale, first_shift, mixing_bias, second_scale, second_shift, shrink_bias = (
        v.reshape(1, width)
        for v in (first_scale, first_shift, mixing_bias, second_scale, second_shift, shrink_bias)
    )

    half = mixing_weight.shape[0] // 2
    piece = swap(lax.dynamic_slice_in_dim(mixing_weight, core * half, half, 0).astype(f32))
    piece_two = lax.ppermute(piece, "dp", cores)
    full_mixing = gather_weight(place, mixing_weight, piece, piece_two)

    joined = (
        heads_weight.reshape(width, 3, pairs, PAIR).transpose(0, 2, 1, 3).reshape(width, 3 * local)
    )
    zero_bias = jnp.zeros((pairs, PAIR), f32)
    joined_bias = jnp.stack(
        [heads_bias[0].reshape(pairs, PAIR), zero_bias, heads_bias[1].reshape(pairs, PAIR)], axis=1
    ).reshape(1, 3 * local)

    each_image = range(images)
    layer_one, qkv, attended, wide, logsum = zip(
        *[
            attend(
                i, rows, block_input, joined, joined_bias, first_scale,
                first_shift,
            )
            for i in each_image
        ]
    )
    hidden_one, layer_two, upstream, activated, pre_low, expand_sums, shrunk, partial_two = zip(
        *[
            feed(
                i, place, block_input, attended[i],
                swap(wide[i]), full_mixing, mixing_bias,
                second_scale, second_shift, output_grad, expand_weight,
                expand_bias.reshape(1, hidden), shrink_weight,
            )
            for i in each_image
        ]
    )
    shrunk_other = [swap(shrunk[i]) for i in each_image]
    backs, sums = [], []
    for i, (left, right) in enumerate(((activated, upstream), (layer_two, pre_low))):
        own_tile = weight_grad(left, right, chips, 4 * i + 1)
        *back, full = attend_back(
            i, partial_two[i], swap(partial_two[i]),
            hidden_one[i], upstream[i], mixing_weight, qkv[i], logsum[i], joined, block_input,
            second_scale, own_tile, chips, 4 * i + 2,
        )
        backs.append(back)
        sums.append(full)
    shrink_full, expand_full = (s.reshape(-1, s.shape[-1]) for s in sums)
    (
        hidden_grad, hidden_low, stacked, query_bias, value_bias, partial_one, sums_two, sums_one,
    ) = zip(*backs)
    partial_other = [swap(partial_one[i]) for i in each_image]
    small = jnp.concatenate(
        [
            sum(query_bias).reshape(-1),
            sum(value_bias).reshape(-1),
            sum(expand_sums).reshape(-1),
            sum(sums_two).reshape(-1),
            sum(sums_one).reshape(-1),
        ]
    )
    each = -(-small.shape[0] // size)
    chunk = -(-each // (8 * local)) * 8 * local
    small_tiles = jnp.pad(small, (0, each * size - small.shape[0])).reshape(size, each)
    small_tiles = jnp.pad(small_tiles, ((0, 0), (0, chunk - each))).reshape(
        chips, 2, chunk // local, local
    )
    heads_own = heads_grad(layer_one, stacked, attended, hidden_low, small_tiles, chips, 9)
    heads_all = gather_alone(heads_own, chips, 10).reshape(size, -1, local)
    share = width // size
    heads_full = (
        heads_all[:, : 3 * share].reshape(size, 3, share, local).transpose(0, 2, 1, 3)
    ).reshape(width, 3, local)
    end = 3 * share + local * width // (size * local)
    mixing_full = (
        heads_all[:, 3 * share : end]
        .reshape(size, width // local, local // size, local)
        .transpose(0, 2, 1, 3)
    ).reshape(local, width)
    small = heads_all[:, end:].reshape(size, chunk)[:, :each].reshape(-1)

    block_output = input_grad = None
    for i in each_image:
        block_output = finish(
            output_kernel, i, block_input.shape,
            [hidden_one[i], shrunk[i], shrunk_other[i], shrink_bias], block_output,
        )
    for i in each_image:
        input_grad = finish(
            input_kernel, i, block_input.shape,
            [hidden_grad[i], partial_one[i], partial_other[i], block_input, first_scale],
            input_grad,
        )

    parts, at = [], 0
    for count in (2 * local, hidden) + 6 * (width,):
        parts.append(small[at : at + count])
        at += count
    first = jnp.stack(parts[6:8])
    first = first + swap(first)
    return (
        block_output,
        input_grad,
        heads_full,
        parts[0].reshape(2, local),
        mixing_full,
        parts[4],
        parts[2],
        parts[3],
        expand_full,
        parts[1],
        shrink_full,
        parts[5],
        first[0],
        first[1],
    )


def solution(mesh):
    placed = (
        P("dp", None, None),
        P(),
        P(),
        P(None, None, "tensor"),
        P(None, "tensor"),
        P("tensor", None),
        P(),
        P(),
        P(),
        P(None, "tensor"),
        P("tensor"),
        P("tensor", None),
        P(),
        P("dp", None, None),
    )
    return jax.shard_map(
        layer,
        mesh=mesh,
        in_specs=placed,
        out_specs=(
            P("dp", None, None),
            P("dp", None, None),
            P(None, None, "tensor"),
            P(None, "tensor"),
            P("tensor", None),
            P(),
            P(),
            P(),
            P(None, "tensor"),
            P("tensor"),
            P("tensor", None),
            P(),
            P(),
            P(),
        ),
        check_vma=False,
    )
```
